32 devices in a mesh: seq: 8 (over y, x, core), tp: 4 (over z).
Axes of the slice: x: 2, y: 2, z: 4, core: 2. Of those that a mesh axis runs over, the one named last changes fastest.
Arguments:
- queries: bfloat16 [1024, 4096], P('seq', 'tp'), may hold values from -16 to 16
- keyvalues: bfloat16 [2, 1024, 1024], P(None, 'seq', 'tp'), may hold values from -16 to 16
- stretch_order: int32 [8], replicated, may hold values from 0 to 7, each once
- block_table: int32 [8, 8], replicated, may hold values 0 or 1
- proj_weight: bfloat16 [4096, 2048], P('tp'), may hold values from -0.09375 to 0.09375
Outputs:
- projected: bfloat16 [1024, 2048], P('seq', 'tp')
The draws below stay inside these ranges and needn't reach their ends.
Inputs may be any that keep to these rules, and one draw needn't show every extreme that they name: `stretch_order`: every stretch number 0 to 7 appears once. `block_table`: entry [i, j] matters only where j < i.
All inputs are finite; a program needn't handle non-finite values.
Results may differ from the reference program's by a relative error of at most 0.014.
Values may be sent and summed in bfloat16 or wider, within the bound.
A program may use at most 128 MiB of HBM per device.

```python
import jax
import jax.numpy as jnp
from jax import lax

QUERY_HEADS = 32
KEY_VALUE_HEADS = 8
HEAD_SIZE = 128
DOUT = 2048
STRETCH_TOKENS = 128
NCHUNK = 8
SEQUENCE_TOKENS = 1024


def query_key_pair(key):
    base = jax.random.fold_in(key, 11)
    random_seeds = jax.random.split(base, 3)
    queries = jnp.clip(jax.random.normal(random_seeds[0], (SEQUENCE_TOKENS, QUERY_HEADS * HEAD_SIZE), jnp.float32), -4.0, 4.0)
    key_matrix = jnp.clip(jax.random.normal(random_seeds[1], (SEQUENCE_TOKENS, KEY_VALUE_HEADS * HEAD_SIZE), jnp.float32), -4.0, 4.0)
    value_vectors = jnp.clip(jax.random.normal(random_seeds[2], (SEQUENCE_TOKENS, KEY_VALUE_HEADS * HEAD_SIZE), jnp.float32), -4.0, 4.0)
    return (queries, jnp.stack([key_matrix, value_vectors]))


def draw_queries(key, part):
    return query_key_pair(key)[0].astype(jnp.bfloat16)


def draw_keyvalues(key, part):
    return query_key_pair(key)[1].astype(jnp.bfloat16)


def set_ends(drawn, stream_key, low, top_value):
    longest = drawn.shape.index(max(drawn.shape))
    spots = []
    for shift in (0, 1):
        where = [jax.random.randint(jax.random.fold_in(stream_key, axis), (), 0, length) for axis, length in enumerate(drawn.shape)]
        where[longest] = (where[longest] + shift) % drawn.shape[longest]
        spots.append(tuple(where))
    return drawn.at[spots[0]].set(low).at[spots[1]].set(top_value)


def level_of(key, extent, cuts, low, top_value):
    factor_of = 1.0
    for dim, parts in cuts:
        steps = jax.random.uniform(jax.random.fold_in(jax.random.fold_in(key, 6), dim), (parts,), jnp.float32, low / len(cuts), top_value / len(cuts))
        factor_of = factor_of * jnp.repeat(jnp.exp(steps), extent[dim] // parts).reshape((-1,) + (1,) * (len(extent) - 1 - dim))
    return factor_of


def scatter_about(rng, dims, width, limit, pieces=(), kind=jnp.bfloat16):
    values = jax.random.normal(rng, dims, jnp.float32) * width
    if len(pieces) > 0:
        values = level_of(rng, dims, pieces, -0.22, 0.18) * values
    return jnp.clip(values, min=-limit, max=limit).astype(kind)


def setup_inputs(seed: int = 0) -> dict:
    key_of = jax.random.split(jax.random.key(seed), 6)
    queries = draw_queries(jax.random.fold_in(key_of[5], 71), 0)
    keyvalues = draw_keyvalues(jax.random.fold_in(key_of[5], 71), 0)
    stretch_order = jax.random.permutation(key_of[2], NCHUNK).astype(jnp.int32)
    block_table = set_ends((jax.random.randint(key_of[3], (NCHUNK, NCHUNK), 0, 4) < 3).astype(jnp.int32), jax.random.fold_in(key_of[3], 1), 0, 1)
    proj_weight = scatter_about(key_of[4], (QUERY_HEADS * HEAD_SIZE, DOUT), (QUERY_HEADS * HEAD_SIZE) ** -0.5, 0.09375, ((0, 4),))
    return {"queries": queries, "keyvalues": keyvalues, "stretch_order": stretch_order, "block_table": block_table, "proj_weight": proj_weight}


def reference(queries, keyvalues, stretch_order, block_table, proj_weight):
    row_index = jnp.arange(SEQUENCE_TOKENS, dtype=jnp.int32)
    row_stretch = stretch_order[row_index // STRETCH_TOKENS].astype(jnp.int32)
    row_pos = row_stretch * STRETCH_TOKENS + row_index % STRETCH_TOKENS
    group_width = QUERY_HEADS // KEY_VALUE_HEADS
    score_scale = 1.0 / (HEAD_SIZE ** 0.5)
    key_matrix = keyvalues[0].astype(jnp.float32).reshape(SEQUENCE_TOKENS, KEY_VALUE_HEADS, HEAD_SIZE)
    value_matrix = keyvalues[1].astype(jnp.float32).reshape(SEQUENCE_TOKENS, KEY_VALUE_HEADS, HEAD_SIZE)

    def block_out(block_index):
        start = (block_index * STRETCH_TOKENS).astype(jnp.int32)
        query_tile = lax.dynamic_slice_in_dim(queries, start, STRETCH_TOKENS, 0).astype(jnp.float32)
        query_tile = query_tile.reshape(STRETCH_TOKENS, KEY_VALUE_HEADS, group_width, HEAD_SIZE)
        query_stretch = lax.dynamic_slice_in_dim(row_stretch, start, STRETCH_TOKENS, 0)
        query_pos = lax.dynamic_slice_in_dim(row_pos, start, STRETCH_TOKENS, 0)
        table_row = block_table[query_stretch[0]]
        table_hits = table_row[row_stretch]
        same_stretch = (row_stretch[None, :] == query_stretch[:, None]) & (row_pos[None, :] <= query_pos[:, None])
        earlier = (row_stretch[None, :] < query_stretch[:, None]) & (table_hits[None, :] == 1)
        allowed = same_stretch | earlier
        scores = jnp.einsum("tkgd,skd->kgts", query_tile, key_matrix) * score_scale
        scores = jnp.where(allowed, scores, -1e30)
        row_max = jnp.max(scores, axis=-1)
        weights = jnp.where(allowed, jnp.exp(scores - row_max[..., None]), 0.0)
        denominator = jnp.sum(weights, axis=-1)
        rounded = weights.astype(jnp.bfloat16).astype(jnp.float32)
        numerator = jnp.einsum("kgts,skd->kgtd", rounded, value_matrix)
        attended = numerator / denominator[..., None]
        attended = jnp.transpose(attended, (2, 0, 1, 3)).reshape(STRETCH_TOKENS, QUERY_HEADS * HEAD_SIZE)
        return attended.astype(jnp.bfloat16)

    blocks = lax.map(block_out, jnp.arange(NCHUNK, dtype=jnp.int32))
    attention = blocks.reshape(SEQUENCE_TOKENS, QUERY_HEADS * HEAD_SIZE)
    return jnp.dot(attention, proj_weight, preferred_element_type=jnp.float32).astype(jnp.bfloat16)
```

```python
import functools

import jax
import jax.numpy as jnp
from jax import lax
from jax.experimental import pallas as pl
from jax.experimental.pallas import tpu as pltpu
from jax.sharding import PartitionSpec as P

HEAD = 128
MASKED = -1e30
LOG2E = 1.4426950408889634
MESH = pl.DeviceIdType.MESH


def kernel(
    n, tp, q_hbm, kv_hbm, order, table, w_hbm, out_ref,
    q_in, q_rows, k_buf, v_buf, w_buf, run_max, acc, att, parts, got,
    in_sem, k_send, v_send, k_recv, v_recv, k_fwd, v_fwd, p_send, p_recv,
):
    rows = q_in.shape[0]
    kv_heads = k_buf.shape[1] // HEAD
    q_heads = q_in.shape[1] // HEAD
    group = q_heads // kv_heads
    grows = group * rows
    width = got.shape[2]
    chips = n // 2
    me = lax.axis_index("seq")
    mt = lax.axis_index("tp")
    chip = me // 2
    core = me % 2
    partner = chip * 2 + 1 - core

    def slot(ref, s, count=1):
        return ref.at[pl.ds(pl.multiple_of(s * rows, rows), count * rows)]

    own_k = pltpu.make_async_copy(kv_hbm.at[0], slot(k_buf, me), in_sem.at[0])
    own_v = pltpu.make_async_copy(kv_hbm.at[1], slot(v_buf, me), in_sem.at[1])
    load_q = pltpu.make_async_copy(q_hbm, q_in, in_sem.at[2])
    load_w = pltpu.make_async_copy(w_hbm, w_buf, in_sem.at[3])
    own_k.start()
    own_v.start()
    load_q.start()

    barrier = pltpu.get_barrier_semaphore()

    def peer(j):
        return ((chip + j) % chips) * 2 + core

    def each(lo, hi, body):
        if hi - lo <= 8:
            for j in range(lo, hi):
                body(j)
        else:
            lax.fori_loop(lo, hi, lambda j, c: (body(j), c)[1], 0)

    def greet_seq(s):
        pl.semaphore_signal(barrier, inc=1, device_id={"seq": s}, device_id_type=MESH)

    greet_seq(partner)
    each(1, chips, lambda j: greet_seq(peer(j)))
    for j in range(1, tp):
        pl.semaphore_signal(barrier, inc=1, device_id={"tp": (mt + j) % tp}, device_id_type=MESH)

    own_k.wait()
    own_v.wait()
    pl.semaphore_wait(barrier, 1 + (chips - 1) + (tp - 1))

    def remote(buf, s, send, recv, index, target):
        return pltpu.make_async_remote_copy(
            src_ref=slot(buf, s), dst_ref=slot(buf, s),
            send_sem=send.at[index], recv_sem=recv.at[s],
            device_id={"seq": target}, device_id_type=MESH,
        )

    def send_all(j):
        remote(k_buf, me, k_send, k_recv, j, peer(j)).start()
        remote(v_buf, me, v_send, v_recv, j, peer(j)).start()

    remote(k_buf, me, k_fwd, k_recv, 0, partner).start()
    remote(v_buf, me, v_fwd, v_recv, 0, partner).start()
    each(1, chips, send_all)
    load_w.start()

    my_stretch = order[me]
    load_q.wait()
    for h in range(q_heads):
        q_rows[h * rows:(h + 1) * rows, :] = q_in[:, h * HEAD:(h + 1) * HEAD]

    def bias_of(s):
        key_stretch = order[s]
        seen = jnp.logical_and(key_stretch < my_stretch, table[my_stretch, key_stretch] == 1)
        return jnp.where(seen, 0.0, MASKED).astype(jnp.float32)

    lane = lax.broadcasted_iota(jnp.int32, (1, 2 * rows), 1)
    scale = LOG2E / HEAD**0.5

    def attend(pair, first):
        bias = jnp.where(lane < rows, bias_of(pair * 2), bias_of(pair * 2 + 1))
        start = pl.multiple_of(pair * 2 * rows, 2 * rows)
        for g in range(kv_heads):
            cols = slice(g * HEAD, (g + 1) * HEAD)
            here = slice(g * grows, (g + 1) * grows)
            keys = k_buf[pl.ds(start, 2 * rows), cols]
            values = v_buf[pl.ds(start, 2 * rows), cols]
            scores = lax.dot_general(
                q_rows[here, :], keys, (((1,), (1,)), ((), ())),
                preferred_element_type=jnp.float32,
            )
            if first:
                q_pos = lax.broadcasted_iota(jnp.int32, (grows, 2 * rows), 0) % rows
                k_col = lax.broadcasted_iota(jnp.int32, (grows, 2 * rows), 1)
                k_pos = k_col - core * rows
                own = (k_pos >= 0) & (k_pos < rows)
                scores = jnp.where(
                    own, jnp.where(k_pos <= q_pos, scores, MASKED), scores + bias
                )
            else:
                scores = scores + bias
            top = jnp.max(scores, axis=1, keepdims=True)
            if first:
                new_max = top
            else:
                old_max = run_max[here, 0:1]
                new_max = jnp.maximum(old_max, top)
            weights = jnp.exp2((scores - new_max) * scale).astype(jnp.bfloat16)
            wide = jnp.concatenate([values, jnp.ones_like(values)], axis=1)
            added = jnp.dot(weights, wide, preferred_element_type=jnp.float32)
            if first:
                acc[here, :] = added
            else:
                acc[here, :] = acc[here, :] * jnp.exp2((old_max - new_max) * scale) + added
            run_max[here, :] = jnp.broadcast_to(new_max, (grows, HEAD))

    def wait_slot(s):
        remote(k_buf, s, k_fwd, k_recv, 0, partner).wait_recv()
        remote(v_buf, s, v_fwd, v_recv, 0, partner).wait_recv()

    wait_slot(partner)
    attend(chip, True)

    def step(j):
        s = ((chip - j + chips) % chips) * 2 + core
        other = ((chip - j + chips) % chips) * 2 + 1 - core
        remote(k_buf, s, k_fwd, k_recv, j, partner).wait_recv()
        remote(k_buf, s, k_fwd, k_recv, j, partner).start()
        remote(v_buf, s, v_fwd, v_recv, j, partner).wait_recv()
        remote(v_buf, s, v_fwd, v_recv, j, partner).start()
        wait_slot(other)
        attend((chip - j + chips) % chips, False)

    each(1, chips, step)

    for h in range(q_heads):
        here = slice(h * rows, (h + 1) * rows)
        att[:, h * HEAD:(h + 1) * HEAD] = (
            acc[here, :HEAD] / acc[here, HEAD:]
        ).astype(jnp.bfloat16)

    load_w.wait()

    def project(t):
        return jnp.dot(
            att[...], w_buf[:, pl.ds(pl.multiple_of(t * width, width), width)],
            preferred_element_type=jnp.float32,
        )

    def part_copy(j, source, target):
        return pltpu.make_async_remote_copy(
            src_ref=parts.at[j], dst_ref=got.at[source],
            send_sem=p_send.at[j], recv_sem=p_recv.at[source],
            device_id={"tp": target}, device_id_type=MESH,
        )

    ahead = sorted(range(1, tp), key=lambda j: -min(j, tp - j))
    for j in ahead:
        t = (mt + j) % tp
        parts[j] = project(t).astype(jnp.bfloat16)
        part_copy(j, mt, t).start()
    total = project(mt)
    for j in reversed(ahead):
        source = (mt + j) % tp
        part_copy(j, source, source).wait_recv()
        total = total + got[source].astype(jnp.float32)
    out_ref[...] = total.astype(out_ref.dtype)

    def drain(j):
        remote(k_buf, me, k_send, k_recv, j, peer(j)).wait_send()
        remote(v_buf, me, v_send, v_recv, j, peer(j)).wait_send()

    def drain_fwd(j):
        remote(k_buf, me, k_fwd, k_recv, j, partner).wait_send()
        remote(v_buf, me, v_fwd, v_recv, j, partner).wait_send()

    each(1, chips, drain)
    each(0, chips, drain_fwd)
    for j in ahead:
        part_copy(j, mt, (mt + j) % tp).wait_send()


def solution(mesh):
    n, tp = mesh.shape["seq"], mesh.shape["tp"]

    def per_device(queries, keyvalues, stretch_order, block_table, proj_weight):
        rows, q_width = queries.shape
        kv_width = keyvalues.shape[2]
        dout = proj_weight.shape[1]
        q_heads = q_width // HEAD
        dma = pltpu.SemaphoreType.DMA
        return pl.pallas_call(
            functools.partial(kernel, n, tp),
            out_shape=jax.ShapeDtypeStruct((rows, dout // tp), jnp.bfloat16),
            in_specs=[
                pl.BlockSpec(memory_space=pl.ANY),
                pl.BlockSpec(memory_space=pl.ANY),
                pl.BlockSpec(memory_space=pltpu.SMEM),
                pl.BlockSpec(memory_space=pltpu.SMEM),
                pl.BlockSpec(memory_space=pl.ANY),
            ],
            out_specs=pl.BlockSpec(memory_space=pltpu.VMEM),
            scratch_shapes=[
                pltpu.VMEM((rows, q_width), jnp.bfloat16),
                pltpu.VMEM((q_heads * rows, HEAD), jnp.bfloat16),
                pltpu.VMEM((n * rows, kv_width), jnp.bfloat16),
                pltpu.VMEM((n * rows, kv_width), jnp.bfloat16),
                pltpu.VMEM(proj_weight.shape, jnp.bfloat16),
                pltpu.VMEM((q_heads * rows, HEAD), jnp.float32),
                pltpu.VMEM((q_heads * rows, 2 * HEAD), jnp.float32),
                pltpu.VMEM((rows, q_width), jnp.bfloat16),
                pltpu.VMEM((tp, rows, dout // tp), jnp.bfloat16),
                pltpu.VMEM((tp, rows, dout // tp), jnp.bfloat16),
                dma((4,)),
                dma((n // 2,)), dma((n // 2,)),
                dma((n,)), dma((n,)),
                dma((n // 2,)), dma((n // 2,)),
                dma((tp,)), dma((tp,)),
            ],
            compiler_params=pltpu.CompilerParams(collective_id=0, has_side_effects=True),
        )(queries, keyvalues, stretch_order, block_table, proj_weight)

    return jax.shard_map(
        per_device, mesh=mesh,
        in_specs=(P("seq", "tp"), P(None, "seq", "tp"), P(), P(), P("tp", None)),
        out_specs=P("seq", "tp"), check_vma=False,
    )
```

```python
import functools

import jax
import jax.numpy as jnp
from jax import lax
from jax.experimental import pallas as pl
from jax.experimental.pallas import tpu as pltpu
from jax.sharding import PartitionSpec as P

HEAD = 128
MASKED = -1e30
LOG2E = 1.4426950408889634
MESH = pl.DeviceIdType.MESH


def kernel(
    n, tp, q_hbm, kv_hbm, order, table, w_hbm, out_ref,
    q_in, q_rows, k_buf, v_buf, w_buf, run_max, acc, att, parts, got, relay,
    in_sem, k_send, v_send, k_recv, v_recv, k_fwd, v_fwd, p_send, p_recv, r_recv,
):
    rows = q_in.shape[0]
    kv_heads = k_buf.shape[1] // HEAD
    q_heads = q_in.shape[1] // HEAD
    group = q_heads // kv_heads
    grows = group * rows
    width = got.shape[2]
    chips = n // 2
    me = lax.axis_index("seq")
    mt = lax.axis_index("tp")
    chip = me // 2
    core = me % 2
    partner = chip * 2 + 1 - core

    def slot(ref, s, count=1):
        return ref.at[pl.ds(pl.multiple_of(s * rows, rows), count * rows)]

    own_k = pltpu.make_async_copy(kv_hbm.at[0], slot(k_buf, me), in_sem.at[0])
    own_v = pltpu.make_async_copy(kv_hbm.at[1], slot(v_buf, me), in_sem.at[1])
    load_q = pltpu.make_async_copy(q_hbm, q_in, in_sem.at[2])
    load_w = pltpu.make_async_copy(w_hbm, w_buf, in_sem.at[3])
    own_k.start()
    own_v.start()
    load_q.start()
    load_w.start()

    barrier = pltpu.get_barrier_semaphore()

    def peer(j):
        return ((chip + j) % chips) * 2 + core

    def each(lo, hi, body):
        if hi - lo <= 8:
            for j in range(lo, hi):
                body(j)
        else:
            lax.fori_loop(lo, hi, lambda j, c: (body(j), c)[1], 0)

    def greet_seq(s):
        pl.semaphore_signal(barrier, inc=1, device_id={"seq": s}, device_id_type=MESH)

    def greet_tp(t):
        pl.semaphore_signal(barrier, inc=1, device_id={"tp": t}, device_id_type=MESH)

    square = chips == 4
    chip_x, chip_y = chip % 2, chip // 2
    xn = (chip_y * 2 + 1 - chip_x) * 2 + core
    yn = ((1 - chip_y) * 2 + chip_x) * 2 + core
    dn = ((1 - chip_y) * 2 + 1 - chip_x) * 2 + core
    line = tp == 4
    side = mt // 2
    inner = mt % 2 * (1 - side) + (1 - mt % 2) * side

    def mirror(d):
        return d * (1 - side) + (3 - d) * side

    greet_seq(partner)
    if square:
        greet_seq(xn)
        greet_seq(yn)
        seq_peers = 3
    else:
        each(1, chips, lambda j: greet_seq(peer(j)))
        seq_peers = chips
    if line:
        greet_tp(mirror(2))
        greet_tp(mirror(1 - inner))

        @pl.when(inner == 1)
        def _():
            greet_tp(mirror(3))

        tp_peers = 2 + inner
    else:
        for j in range(1, tp):
            greet_tp((mt + j) % tp)
        tp_peers = tp - 1

    own_k.wait()
    own_v.wait()
    pl.semaphore_wait(barrier, seq_peers + tp_peers)

    def remote(buf, s, send, recv, index, target):
        return pltpu.make_async_remote_copy(
            src_ref=slot(buf, s), dst_ref=slot(buf, s),
            send_sem=send.at[index], recv_sem=recv.at[s],
            device_id={"seq": target}, device_id_type=MESH,
        )

    def send_all(j):
        remote(k_buf, me, k_send, k_recv, j, peer(j)).start()
        remote(v_buf, me, v_send, v_recv, j, peer(j)).start()

    remote(k_buf, me, k_fwd, k_recv, 0, partner).start()
    remote(v_buf, me, v_fwd, v_recv, 0, partner).start()
    if square:
        remote(k_buf, me, k_send, k_recv, 0, xn).start()
        remote(v_buf, me, v_send, v_recv, 0, yn).start()
        remote(v_buf, me, v_send, v_recv, 1, xn).start()
        remote(k_buf, me, k_send, k_recv, 1, yn).start()
    else:
        each(1, chips, send_all)

    my_stretch = order[me]
    load_q.wait()
    for h in range(q_heads):
        q_rows[h * rows:(h + 1) * rows, :] = q_in[:, h * HEAD:(h + 1) * HEAD]

    def bias_of(s):
        key_stretch = order[s]
        seen = jnp.logical_and(key_stretch < my_stretch, table[my_stretch, key_stretch] == 1)
        return jnp.where(seen, 0.0, MASKED).astype(jnp.float32)

    lane = lax.broadcasted_iota(jnp.int32, (1, 2 * rows), 1)
    scale = LOG2E / HEAD**0.5

    def attend(first_slot, count, first):
        if count == 2:
            bias = jnp.where(lane < rows, bias_of(first_slot), bias_of(first_slot + 1))
        else:
            bias = bias_of(first_slot)
        start = pl.multiple_of(first_slot * rows, rows)
        for g in range(kv_heads):
            cols = slice(g * HEAD, (g + 1) * HEAD)
            here = slice(g * grows, (g + 1) * grows)
            keys = k_buf[pl.ds(start, count * rows), cols]
            values = v_buf[pl.ds(start, count * rows), cols]
            scores = lax.dot_general(
                q_rows[here, :], keys, (((1,), (1,)), ((), ())),
                preferred_element_type=jnp.float32,
            )
            if first:
                q_pos = lax.broadcasted_iota(jnp.int32, (grows, 2 * rows), 0) % rows
                k_col = lax.broadcasted_iota(jnp.int32, (grows, 2 * rows), 1)
                k_pos = k_col - core * rows
                own = (k_pos >= 0) & (k_pos < rows)
                scores = jnp.where(
                    own, jnp.where(k_pos <= q_pos, scores, MASKED), scores + bias
                )
            else:
                scores = scores + bias
            top = jnp.max(scores, axis=1, keepdims=True)
            if first:
                new_max = top
            else:
                old_max = run_max[here, 0:1]
                new_max = jnp.maximum(old_max, top)
            weights = jnp.exp2((scores - new_max) * scale).astype(jnp.bfloat16)
            wide = jnp.concatenate([values, jnp.ones_like(values)], axis=1)
            added = jnp.dot(weights, wide, preferred_element_type=jnp.float32)
            if first:
                acc[here, :] = added
            else:
                acc[here, :] = acc[here, :] * jnp.exp2((old_max - new_max) * scale) + added
            run_max[here, :] = jnp.broadcast_to(new_max, (grows, HEAD))

    def wait_slot(s):
        remote(k_buf, s, k_fwd, k_recv, 0, partner).wait_recv()
        remote(v_buf, s, v_fwd, v_recv, 0, partner).wait_recv()

    wait_slot(partner)
    attend(chip * 2, 2, True)

    def step(j):
        s = ((chip - j + chips) % chips) * 2 + core
        other = ((chip - j + chips) % chips) * 2 + 1 - core
        remote(k_buf, s, k_fwd, k_recv, j, partner).wait_recv()
        remote(k_buf, s, k_fwd, k_recv, j, partner).start()
        remote(v_buf, s, v_fwd, v_recv, j, partner).wait_recv()
        remote(v_buf, s, v_fwd, v_recv, j, partner).start()
        wait_slot(other)
        attend(s - core, 2, False)

    def arrive(buf, recv, fwd, s, j, onward=None, send=None):
        remote(buf, s, fwd, recv, j, partner).wait_recv()
        if onward is not None:
            remote(buf, s, send, recv, 2, onward).start()
        remote(buf, s, fwd, recv, j, partner).start()

    if square:
        arrive(k_buf, k_recv, k_fwd, xn, 1, yn, k_send)
        arrive(v_buf, v_recv, v_fwd, yn, 2, xn, v_send)
        arrive(v_buf, v_recv, v_fwd, xn, 1)
        arrive(k_buf, k_recv, k_fwd, yn, 2)
        wait_slot(xn + 1 - 2 * core)
        attend(xn - core, 2, False)
        wait_slot(yn + 1 - 2 * core)
        attend(yn - core, 2, False)
        arrive(k_buf, k_recv, k_fwd, dn, 3)
        arrive(v_buf, v_recv, v_fwd, dn, 3)
        attend(dn, 1, False)
        wait_slot(dn + 1 - 2 * core)
        attend(dn + 1 - 2 * core, 1, False)
    else:
        each(1, chips, step)

    for h in range(q_heads):
        here = slice(h * rows, (h + 1) * rows)
        att[:, h * HEAD:(h + 1) * HEAD] = (
            acc[here, :HEAD] / acc[here, HEAD:]
        ).astype(jnp.bfloat16)

    load_w.wait()

    def project(t):
        return jnp.dot(
            att[...], w_buf[:, pl.ds(pl.multiple_of(t * width, width), width)],
            preferred_element_type=jnp.float32,
        )

    def part_copy(j, source, target):
        return pltpu.make_async_remote_copy(
            src_ref=parts.at[j], dst_ref=got.at[source],
            send_sem=p_send.at[j], recv_sem=p_recv.at[source],
            device_id={"tp": target}, device_id_type=MESH,
        )

    def half_copy(i, dst, recv, target):
        piece = pl.ds(i * (rows // 2), rows // 2)
        return pltpu.make_async_remote_copy(
            src_ref=parts.at[2, piece], dst_ref=dst.at[piece],
            send_sem=p_send.at[2 + i], recv_sem=recv,
            device_id={"tp": target}, device_id_type=MESH,
        )

    if line:
        m0, m1, m2, m3 = (mirror(d) for d in range(4))

        @pl.when(inner == 0)
        def _():
            parts[2] = project(m3).astype(jnp.bfloat16)
            for i in range(2):
                half_copy(i, relay, r_recv.at[i], m1).start()
            parts[0] = project(m2).astype(jnp.bfloat16)
            part_copy(0, mt, m2).start()
            parts[1] = project(m1).astype(jnp.bfloat16)
            part_copy(1, mt, m1).start()
            total = project(mt)
            part_copy(0, m1, m1).wait_recv()
            total = total + got[m1].astype(jnp.float32)
            for i in range(2):
                half_copy(i, got.at[m2], r_recv.at[i], m2).wait_recv()
            total = total + got[m2].astype(jnp.float32)
            out_ref[...] = total.astype(out_ref.dtype)

        @pl.when(inner == 1)
        def _():
            parts[0] = project(m2).astype(jnp.bfloat16)
            part_copy(0, mt, m2).start()
            parts[1] = project(m0).astype(jnp.bfloat16)
            part_copy(1, mt, m0).start()
            far = project(m3)
            total = project(mt)
            for i in range(2):
                piece = slice(i * (rows // 2), (i + 1) * (rows // 2))
                half_copy(i, relay, r_recv.at[i], m0).wait_recv()
                parts[2, piece] = (far[piece] + relay[piece].astype(jnp.float32)).astype(jnp.bfloat16)
                half_copy(i, got.at[mt], r_recv.at[i], m3).start()
            for source in (m2, m3, m0):
                part_copy(0, source, source).wait_recv()
                total = total + got[source].astype(jnp.float32)
            out_ref[...] = total.astype(out_ref.dtype)

        part_copy(0, mt, m2).wait_send()
        part_copy(1, mt, m0).wait_send()
        for i in range(2):
            half_copy(i, relay, r_recv.at[i], m1).wait_send()
    else:
        ahead = sorted(range(1, tp), key=lambda j: -min(j, tp - j))
        for j in ahead:
            t = (mt + j) % tp
            parts[j] = project(t).astype(jnp.bfloat16)
            part_copy(j, mt, t).start()
        total = project(mt)
        for j in reversed(ahead):
            source = (mt + j) % tp
            part_copy(j, source, source).wait_recv()
            total = total + got[source].astype(jnp.float32)
        out_ref[...] = total.astype(out_ref.dtype)
        for j in ahead:
            part_copy(j, mt, (mt + j) % tp).wait_send()

    def drain(j):
        remote(k_buf, me, k_send, k_recv, j, peer(j)).wait_send()
        remote(v_buf, me, v_send, v_recv, j, peer(j)).wait_send()

    def drain_fwd(j):
        remote(k_buf, me, k_fwd, k_recv, j, partner).wait_send()
        remote(v_buf, me, v_fwd, v_recv, j, partner).wait_send()

    if square:
        for j in range(3):
            remote(k_buf, me, k_send, k_recv, j, yn).wait_send()
            remote(v_buf, me, v_send, v_recv, j, xn).wait_send()
    else:
        each(1, chips, drain)
    each(0, chips, drain_fwd)


def solution(mesh):
    n, tp = mesh.shape["seq"], mesh.shape["tp"]

    def per_device(queries, keyvalues, stretch_order, block_table, proj_weight):
        rows, q_width = queries.shape
        kv_width = keyvalues.shape[2]
        dout = proj_weight.shape[1]
        q_heads = q_width // HEAD
        dma = pltpu.SemaphoreType.DMA
        return pl.pallas_call(
            functools.partial(kernel, n, tp),
            out_shape=jax.ShapeDtypeStruct((rows, dout // tp), jnp.bfloat16),
            in_specs=[
                pl.BlockSpec(memory_space=pl.ANY),
                pl.BlockSpec(memory_space=pl.ANY),
                pl.BlockSpec(memory_space=pltpu.SMEM),
                pl.BlockSpec(memory_space=pltpu.SMEM),
                pl.BlockSpec(memory_space=pl.ANY),
            ],
            out_specs=pl.BlockSpec(memory_space=pltpu.VMEM),
            scratch_shapes=[
                pltpu.VMEM((rows, q_width), jnp.bfloat16),
                pltpu.VMEM((q_heads * rows, HEAD), jnp.bfloat16),
                pltpu.VMEM((n * rows, kv_width), jnp.bfloat16),
                pltpu.VMEM((n * rows, kv_width), jnp.bfloat16),
                pltpu.VMEM(proj_weight.shape, jnp.bfloat16),
                pltpu.VMEM((q_heads * rows, HEAD), jnp.float32),
                pltpu.VMEM((q_heads * rows, 2 * HEAD), jnp.float32),
                pltpu.VMEM((rows, q_width), jnp.bfloat16),
                pltpu.VMEM((tp, rows, dout // tp), jnp.bfloat16),
                pltpu.VMEM((tp, rows, dout // tp), jnp.bfloat16),
                pltpu.VMEM((rows, dout // tp), jnp.bfloat16),
                dma((4,)),
                dma((n // 2,)), dma((n // 2,)),
                dma((n,)), dma((n,)),
                dma((n // 2,)), dma((n // 2,)),
                dma((max(tp, 4),)), dma((tp,)), dma((2,)),
            ],
            compiler_params=pltpu.CompilerParams(collective_id=0, has_side_effects=True),
        )(queries, keyvalues, stretch_order, block_table, proj_weight)

    return jax.shard_map(
        per_device, mesh=mesh,
        in_specs=(P("seq", "tp"), P(None, "seq", "tp"), P(), P(), P("tp", None)),
        out_specs=P("seq", "tp"), check_vma=False,
    )
```

```python
import functools

import jax
import jax.numpy as jnp
from jax import lax
from jax.experimental import pallas as pl
from jax.experimental.pallas import tpu as pltpu
from jax.sharding import PartitionSpec as P

HEAD = 128
MASKED = -1e30
LOG2E = 1.4426950408889634
MESH = pl.DeviceIdType.MESH


def kernel(
    n, tp, q_hbm, kv_hbm, order_hbm, table_hbm, w_hbm, out_ref,
    order, table, q_in, q_rows, k_buf, v_buf, w_buf, run_max, acc, att, parts, got, relay,
    in_sem, k_send, v_send, k_recv, v_recv, k_fwd, v_fwd, p_send, p_recv, r_recv,
):
    rows = q_in.shape[0]
    kv_heads = k_buf.shape[1] // HEAD
    q_heads = q_in.shape[1] // HEAD
    group = q_heads // kv_heads
    grows = group * rows
    width = got.shape[2]
    chips = n // 2
    me = lax.axis_index("seq")
    mt = lax.axis_index("tp")
    chip = me // 2
    core = me % 2
    partner = chip * 2 + 1 - core

    def slot(ref, s, count=1):
        return ref.at[pl.ds(pl.multiple_of(s * rows, rows), count * rows)]

    own_k = pltpu.make_async_copy(kv_hbm.at[0], slot(k_buf, me), in_sem.at[0])
    own_v = pltpu.make_async_copy(kv_hbm.at[1], slot(v_buf, me), in_sem.at[1])
    load_q = pltpu.make_async_copy(q_hbm, q_in, in_sem.at[2])
    load_w = pltpu.make_async_copy(w_hbm, w_buf, in_sem.at[3])
    own_k.start()
    own_v.start()
    load_q.start()
    load_order = pltpu.make_async_copy(order_hbm, order, in_sem.at[4])
    load_table = pltpu.make_async_copy(table_hbm, table, in_sem.at[5])
    load_order.start()
    load_table.start()
    load_w.start()

    barrier = pltpu.get_barrier_semaphore()

    def peer(j):
        return ((chip + j) % chips) * 2 + core

    def each(lo, hi, body):
        if hi - lo <= 8:
            for j in range(lo, hi):
                body(j)
        else:
            lax.fori_loop(lo, hi, lambda j, c: (body(j), c)[1], 0)

    def greet_seq(s):
        pl.semaphore_signal(barrier, inc=1, device_id={"seq": s}, device_id_type=MESH)

    def greet_tp(t):
        pl.semaphore_signal(barrier, inc=1, device_id={"tp": t}, device_id_type=MESH)

    square = chips == 4
    chip_x, chip_y = chip % 2, chip // 2
    xn = (chip_y * 2 + 1 - chip_x) * 2 + 1 - core
    yn = ((1 - chip_y) * 2 + chip_x) * 2 + 1 - core
    dn = ((1 - chip_y) * 2 + 1 - chip_x) * 2 + core
    line = tp == 4
    side = mt // 2
    inner = mt % 2 * (1 - side) + (1 - mt % 2) * side

    def mirror(d):
        return d * (1 - side) + (3 - d) * side

    greet_seq(partner)
    if square:
        greet_seq(xn)
        greet_seq(yn)
        seq_peers = 3
    else:
        each(1, chips, lambda j: greet_seq(peer(j)))
        seq_peers = chips
    if line:
        greet_tp(mirror(2))
        greet_tp(mirror(1 - inner))

        @pl.when(inner == 1)
        def _():
            greet_tp(mirror(3))

        tp_peers = 2 + inner
    else:
        for j in range(1, tp):
            greet_tp((mt + j) % tp)
        tp_peers = tp - 1

    own_k.wait()
    own_v.wait()
    pl.semaphore_wait(barrier, seq_peers + tp_peers)

    def remote(buf, s, send, recv, index, target):
        return pltpu.make_async_remote_copy(
            src_ref=slot(buf, s), dst_ref=slot(buf, s),
            send_sem=send.at[index], recv_sem=recv.at[s],
            device_id={"seq": target}, device_id_type=MESH,
        )

    def send_all(j):
        remote(k_buf, me, k_send, k_recv, j, peer(j)).start()
        remote(v_buf, me, v_send, v_recv, j, peer(j)).start()

    remote(k_buf, me, k_fwd, k_recv, 0, partner).start()
    remote(v_buf, me, v_fwd, v_recv, 0, partner).start()
    if square:
        remote(k_buf, me, k_send, k_recv, 0, xn).start()
        remote(v_buf, me, v_send, v_recv, 0, yn).start()
        remote(v_buf, me, v_send, v_recv, 1, xn).start()
        remote(k_buf, me, k_send, k_recv, 1, yn).start()
    else:
        each(1, chips, send_all)

    load_q.wait()
    for h in range(q_heads):
        q_rows[h * rows:(h + 1) * rows, :] = q_in[:, h * HEAD:(h + 1) * HEAD]

    def bias_of(s):
        key_stretch = order[s]
        seen = jnp.logical_and(key_stretch < my_stretch, table[my_stretch, key_stretch] == 1)
        return jnp.where(seen, 0.0, MASKED).astype(jnp.float32)

    load_order.wait()
    load_table.wait()
    my_stretch = order[me]
    scale = LOG2E / HEAD**0.5

    def attend(slots, first=False):
        count = len(slots)

        def rows_of(buf, cols):
            return jnp.concatenate(
                [buf[pl.ds(pl.multiple_of(s * rows, rows), rows), cols] for s in slots], axis=0
            )

        bias = jnp.concatenate(
            [jnp.full((1, rows), bias_of(s), jnp.float32) for s in slots], axis=1
        )
        for g in range(kv_heads):
            cols = slice(g * HEAD, (g + 1) * HEAD)
            here = slice(g * grows, (g + 1) * grows)
            keys = rows_of(k_buf, cols)
            values = rows_of(v_buf, cols)
            scores = lax.dot_general(
                q_rows[here, :], keys, (((1,), (1,)), ((), ())),
                preferred_element_type=jnp.float32,
            )
            if first:
                shape = (grows, count * rows)
                q_pos = lax.broadcasted_iota(jnp.int32, shape, 0) % rows
                k_pos = lax.broadcasted_iota(jnp.int32, shape, 1)
                scores = jnp.where(
                    k_pos < rows, jnp.where(k_pos <= q_pos, scores, MASKED), scores + bias
                )
            else:
                scores = scores + bias
            top = jnp.max(scores, axis=1, keepdims=True)
            if first:
                new_max = top
            else:
                old_max = run_max[here, 0:1]
                new_max = jnp.maximum(old_max, top)
            weights = jnp.exp2((scores - new_max) * scale).astype(jnp.bfloat16)
            wide = jnp.concatenate([values, jnp.ones_like(values)], axis=1)
            added = jnp.dot(weights, wide, preferred_element_type=jnp.float32)
            if first:
                acc[here, :] = added
            else:
                acc[here, :] = acc[here, :] * jnp.exp2((old_max - new_max) * scale) + added
            run_max[here, :] = jnp.broadcast_to(new_max, (grows, HEAD))

    def wait_slot(s):
        remote(k_buf, s, k_fwd, k_recv, 0, partner).wait_recv()
        remote(v_buf, s, v_fwd, v_recv, 0, partner).wait_recv()

    wait_slot(partner)
    attend([me, partner], True)

    def step(j):
        s = ((chip - j + chips) % chips) * 2 + core
        other = ((chip - j + chips) % chips) * 2 + 1 - core
        remote(k_buf, s, k_fwd, k_recv, j, partner).wait_recv()
        remote(k_buf, s, k_fwd, k_recv, j, partner).start()
        remote(v_buf, s, v_fwd, v_recv, j, partner).wait_recv()
        remote(v_buf, s, v_fwd, v_recv, j, partner).start()
        wait_slot(other)
        attend([s, other])

    def arrive(buf, recv, fwd, s, j, onward=None, send=None):
        remote(buf, s, fwd, recv, j, partner).wait_recv()
        if onward is not None:
            remote(buf, s, send, recv, 2, onward).start()
        remote(buf, s, fwd, recv, j, partner).start()

    if square:
        arrive(k_buf, k_recv, k_fwd, xn, 1, yn, k_send)
        arrive(v_buf, v_recv, v_fwd, yn, 2, xn, v_send)
        arrive(v_buf, v_recv, v_fwd, xn, 1)
        arrive(k_buf, k_recv, k_fwd, yn, 2)
        attend([xn, yn])
        arrive(k_buf, k_recv, k_fwd, dn, 3)
        arrive(v_buf, v_recv, v_fwd, dn, 3)
        xo, yo, do = xn - 1 + 2 * core, yn - 1 + 2 * core, dn + 1 - 2 * core
        wait_slot(xo)
        wait_slot(yo)
        attend([xo, yo, dn])
        wait_slot(do)
        attend([do])
    else:
        each(1, chips, step)

    for h in range(q_heads):
        here = slice(h * rows, (h + 1) * rows)
        att[:, h * HEAD:(h + 1) * HEAD] = (
            acc[here, :HEAD] / acc[here, HEAD:]
        ).astype(jnp.bfloat16)

    load_w.wait()

    def project(t):
        return jnp.dot(
            att[...], w_buf[:, pl.ds(pl.multiple_of(t * width, width), width)],
            preferred_element_type=jnp.float32,
        )

    def part_copy(j, source, target):
        return pltpu.make_async_remote_copy(
            src_ref=parts.at[j], dst_ref=got.at[source],
            send_sem=p_send.at[j], recv_sem=p_recv.at[source],
            device_id={"tp": target}, device_id_type=MESH,
        )

    def half_copy(i, dst, recv, target):
        piece = pl.ds(i * (rows // 2), rows // 2)
        return pltpu.make_async_remote_copy(
            src_ref=parts.at[2, piece], dst_ref=dst.at[piece],
            send_sem=p_send.at[2 + i], recv_sem=recv,
            device_id={"tp": target}, device_id_type=MESH,
        )

    if line:
        m0, m1, m2, m3 = (mirror(d) for d in range(4))

        @pl.when(inner == 0)
        def _():
            parts[2] = project(m3).astype(jnp.bfloat16)
            for i in range(2):
                half_copy(i, relay, r_recv.at[i], m1).start()
            parts[0] = project(m2).astype(jnp.bfloat16)
            part_copy(0, mt, m2).start()
            parts[1] = project(m1).astype(jnp.bfloat16)
            part_copy(1, mt, m1).start()
            total = project(mt)
            part_copy(0, m1, m1).wait_recv()
            total = total + got[m1].astype(jnp.float32)
            for i in range(2):
                half_copy(i, got.at[m2], r_recv.at[i], m2).wait_recv()
            total = total + got[m2].astype(jnp.float32)
            out_ref[...] = total.astype(out_ref.dtype)

        @pl.when(inner == 1)
        def _():
            parts[0] = project(m2).astype(jnp.bfloat16)
            part_copy(0, mt, m2).start()
            parts[1] = project(m0).astype(jnp.bfloat16)
            part_copy(1, mt, m0).start()
            far = project(m3)
            total = project(mt)
            for i in range(2):
                piece = slice(i * (rows // 2), (i + 1) * (rows // 2))
                half_copy(i, relay, r_recv.at[i], m0).wait_recv()
                parts[2, piece] = (far[piece] + relay[piece].astype(jnp.float32)).astype(jnp.bfloat16)
                half_copy(i, got.at[mt], r_recv.at[i], m3).start()
            for source in (m2, m3, m0):
                part_copy(0, source, source).wait_recv()
                total = total + got[source].astype(jnp.float32)
            out_ref[...] = total.astype(out_ref.dtype)

        part_copy(0, mt, m2).wait_send()
        part_copy(1, mt, m0).wait_send()
        for i in range(2):
            half_copy(i, relay, r_recv.at[i], m1).wait_send()
    else:
        ahead = sorted(range(1, tp), key=lambda j: -min(j, tp - j))
        for j in ahead:
            t = (mt + j) % tp
            parts[j] = project(t).astype(jnp.bfloat16)
            part_copy(j, mt, t).start()
        total = project(mt)
        for j in reversed(ahead):
            source = (mt + j) % tp
            part_copy(j, source, source).wait_recv()
            total = total + got[source].astype(jnp.float32)
        out_ref[...] = total.astype(out_ref.dtype)
        for j in ahead:
            part_copy(j, mt, (mt + j) % tp).wait_send()

    def drain(j):
        remote(k_buf, me, k_send, k_recv, j, peer(j)).wait_send()
        remote(v_buf, me, v_send, v_recv, j, peer(j)).wait_send()

    def drain_fwd(j):
        remote(k_buf, me, k_fwd, k_recv, j, partner).wait_send()
        remote(v_buf, me, v_fwd, v_recv, j, partner).wait_send()

    if square:
        for j in range(3):
            remote(k_buf, me, k_send, k_recv, j, yn).wait_send()
            remote(v_buf, me, v_send, v_recv, j, xn).wait_send()
    else:
        each(1, chips, drain)
    each(0, chips, drain_fwd)


def solution(mesh):
    n, tp = mesh.shape["seq"], mesh.shape["tp"]

    def per_device(queries, keyvalues, stretch_order, block_table, proj_weight):
        rows, q_width = queries.shape
        kv_width = keyvalues.shape[2]
        dout = proj_weight.shape[1]
        q_heads = q_width // HEAD
        dma = pltpu.SemaphoreType.DMA
        return pl.pallas_call(
            functools.partial(kernel, n, tp),
            out_shape=jax.ShapeDtypeStruct((rows, dout // tp), jnp.bfloat16),
            in_specs=[
                pl.BlockSpec(memory_space=pl.ANY),
                pl.BlockSpec(memory_space=pl.ANY),
                pl.BlockSpec(memory_space=pl.ANY),
                pl.BlockSpec(memory_space=pl.ANY),
                pl.BlockSpec(memory_space=pl.ANY),
            ],
            out_specs=pl.BlockSpec(memory_space=pltpu.VMEM),
            scratch_shapes=[
                pltpu.SMEM(stretch_order.shape, jnp.int32),
                pltpu.SMEM(block_table.shape, jnp.int32),
                pltpu.VMEM((rows, q_width), jnp.bfloat16),
                pltpu.VMEM((q_heads * rows, HEAD), jnp.bfloat16),
                pltpu.VMEM((n * rows, kv_width), jnp.bfloat16),
                pltpu.VMEM((n * rows, kv_width), jnp.bfloat16),
                pltpu.VMEM(proj_weight.shape, jnp.bfloat16),
                pltpu.VMEM((q_heads * rows, HEAD), jnp.float32),
                pltpu.VMEM((q_heads * rows, 2 * HEAD), jnp.float32),
                pltpu.VMEM((rows, q_width), jnp.bfloat16),
                pltpu.VMEM((tp, rows, dout // tp), jnp.bfloat16),
                pltpu.VMEM((tp, rows, dout // tp), jnp.bfloat16),
                pltpu.VMEM((rows, dout // tp), jnp.bfloat16),
                dma((6,)),
                dma((n // 2,)), dma((n // 2,)),
                dma((n,)), dma((n,)),
                dma((n // 2,)), dma((n // 2,)),
                dma((max(tp, 4),)), dma((tp,)), dma((2,)),
            ],
            compiler_params=pltpu.CompilerParams(
                collective_id=0, has_side_effects=True,
            ),
        )(queries, keyvalues, stretch_order, block_table, proj_weight)

    return jax.shard_map(
        per_device, mesh=mesh,
        in_specs=(P("seq", "tp"), P(None, "seq", "tp"), P(), P(), P("tp", None)),
        out_specs=P("seq", "tp"), check_vma=False,
    )
```

```python
import functools

import jax
import jax.numpy as jnp
from jax import lax
from jax.experimental import pallas as pl
from jax.experimental.pallas import tpu as pltpu
from jax.sharding import PartitionSpec as P

HEAD = 128
MASKED = -1e30
LOG2E = 1.4426950408889634
MESH = pl.DeviceIdType.MESH


def kernel(
    n, tp, q_hbm, kv_hbm, order_hbm, table_hbm, w_hbm, out_ref,
    order, table, q_in, q_rows, k_buf, v_buf, w_buf, run_max, acc, att, parts, got, relay,
    in_sem, k_send, v_send, k_recv, v_recv, k_fwd, v_fwd, p_send, p_recv, r_recv,
):
    rows = q_in.shape[0]
    kv_heads = k_buf.shape[1] // HEAD
    q_heads = q_in.shape[1] // HEAD
    group = q_heads // kv_heads
    grows = group * rows
    width = got.shape[2]
    chips = n // 2
    me = lax.axis_index("seq")
    mt = lax.axis_index("tp")
    chip = me // 2
    core = me % 2
    partner = chip * 2 + 1 - core

    def slot(ref, s, count=1):
        return ref.at[pl.ds(pl.multiple_of(s * rows, rows), count * rows)]

    own_k = pltpu.make_async_copy(kv_hbm.at[0], slot(k_buf, me), in_sem.at[0])
    own_v = pltpu.make_async_copy(kv_hbm.at[1], slot(v_buf, me), in_sem.at[1])
    load_q = pltpu.make_async_copy(q_hbm, q_in, in_sem.at[2])
    load_w = pltpu.make_async_copy(w_hbm, w_buf, in_sem.at[3])
    own_k.start()
    own_v.start()
    load_q.start()
    load_order = pltpu.make_async_copy(order_hbm, order, in_sem.at[4])
    load_table = pltpu.make_async_copy(table_hbm, table, in_sem.at[5])
    load_order.start()
    load_table.start()
    load_w.start()

    barrier = pltpu.get_barrier_semaphore()

    def peer(j):
        return ((chip + j) % chips) * 2 + core

    def each(lo, hi, body):
        if hi - lo <= 8:
            for j in range(lo, hi):
                body(j)
        else:
            lax.fori_loop(lo, hi, lambda j, c: (body(j), c)[1], 0)

    def greet_seq(s):
        pl.semaphore_signal(barrier, inc=1, device_id={"seq": s}, device_id_type=MESH)

    def greet_tp(t):
        pl.semaphore_signal(barrier, inc=1, device_id={"tp": t}, device_id_type=MESH)

    square = chips == 4
    chip_x, chip_y = chip % 2, chip // 2
    xn = (chip_y * 2 + 1 - chip_x) * 2 + 1 - core
    yn = ((1 - chip_y) * 2 + chip_x) * 2 + 1 - core
    dn = ((1 - chip_y) * 2 + 1 - chip_x) * 2 + core
    line = tp == 4
    side = mt // 2
    inner = mt % 2 * (1 - side) + (1 - mt % 2) * side

    def mirror(d):
        return d * (1 - side) + (3 - d) * side

    greet_seq(partner)
    if square:
        greet_seq(xn)
        greet_seq(yn)
        seq_peers = 3
    else:
        each(1, chips, lambda j: greet_seq(peer(j)))
        seq_peers = chips
    if line:
        greet_tp(mirror(2))
        greet_tp(mirror(1 - inner))

        @pl.when(inner == 1)
        def _():
            greet_tp(mirror(3))

        tp_peers = 2 + inner
    else:
        for j in range(1, tp):
            greet_tp((mt + j) % tp)
        tp_peers = tp - 1

    own_k.wait()
    own_v.wait()
    pl.semaphore_wait(barrier, seq_peers + tp_peers)

    def remote(buf, s, send, recv, index, target):
        return pltpu.make_async_remote_copy(
            src_ref=slot(buf, s), dst_ref=slot(buf, s),
            send_sem=send.at[index], recv_sem=recv.at[s],
            device_id={"seq": target}, device_id_type=MESH,
        )

    def send_all(j):
        remote(k_buf, me, k_send, k_recv, j, peer(j)).start()
        remote(v_buf, me, v_send, v_recv, j, peer(j)).start()

    remote(k_buf, me, k_fwd, k_recv, 0, partner).start()
    remote(v_buf, me, v_fwd, v_recv, 0, partner).start()
    if square:
        remote(k_buf, me, k_send, k_recv, 0, xn).start()
        remote(v_buf, me, v_send, v_recv, 0, yn).start()
        remote(v_buf, me, v_send, v_recv, 1, xn).start()
        remote(k_buf, me, k_send, k_recv, 1, yn).start()
    else:
        each(1, chips, send_all)

    load_q.wait()
    for h in range(q_heads):
        q_rows[h * rows:(h + 1) * rows, :] = q_in[:, h * HEAD:(h + 1) * HEAD]

    def bias_of(s):
        key_stretch = order[s]
        seen = jnp.logical_and(key_stretch < my_stretch, table[my_stretch, key_stretch] == 1)
        return jnp.where(seen, 0.0, MASKED).astype(jnp.float32)

    load_order.wait()
    load_table.wait()
    my_stretch = order[me]
    scale = LOG2E / HEAD**0.5

    def attend(slots, first=False):
        count = len(slots)

        def rows_of(buf, cols):
            return jnp.concatenate(
                [buf[pl.ds(pl.multiple_of(s * rows, rows), rows), cols] for s in slots], axis=0
            )

        bias = jnp.concatenate(
            [jnp.full((1, rows), bias_of(s), jnp.float32) for s in slots], axis=1
        )
        for g in range(kv_heads):
            cols = slice(g * HEAD, (g + 1) * HEAD)
            here = slice(g * grows, (g + 1) * grows)
            keys = rows_of(k_buf, cols)
            values = rows_of(v_buf, cols)
            scores = lax.dot_general(
                q_rows[here, :], keys, (((1,), (1,)), ((), ())),
                preferred_element_type=jnp.float32,
            )
            if first:
                shape = (grows, count * rows)
                q_pos = lax.broadcasted_iota(jnp.int32, shape, 0) % rows
                k_pos = lax.broadcasted_iota(jnp.int32, shape, 1)
                scores = jnp.where(
                    k_pos < rows, jnp.where(k_pos <= q_pos, scores, MASKED), scores + bias
                )
            else:
                scores = scores + bias
            top = jnp.max(scores, axis=1, keepdims=True)
            if first:
                new_max = top
            else:
                old_max = run_max[here, 0:1]
                new_max = jnp.maximum(old_max, top)
            weights = jnp.exp2((scores - new_max) * scale).astype(jnp.bfloat16)
            wide = jnp.concatenate([values, jnp.ones_like(values)], axis=1)
            added = jnp.dot(weights, wide, preferred_element_type=jnp.float32)
            if first:
                acc[here, :] = added
            else:
                acc[here, :] = acc[here, :] * jnp.exp2((old_max - new_max) * scale) + added
            run_max[here, :] = jnp.broadcast_to(new_max, (grows, HEAD))

    def wait_slot(s):
        remote(k_buf, s, k_fwd, k_recv, 0, partner).wait_recv()
        remote(v_buf, s, v_fwd, v_recv, 0, partner).wait_recv()

    wait_slot(partner)
    attend([me, partner], True)

    def step(j):
        s = ((chip - j + chips) % chips) * 2 + core
        other = ((chip - j + chips) % chips) * 2 + 1 - core
        remote(k_buf, s, k_fwd, k_recv, j, partner).wait_recv()
        remote(k_buf, s, k_fwd, k_recv, j, partner).start()
        remote(v_buf, s, v_fwd, v_recv, j, partner).wait_recv()
        remote(v_buf, s, v_fwd, v_recv, j, partner).start()
        wait_slot(other)
        attend([s, other])

    def arrive(buf, recv, fwd, s, j, onward=None, send=None):
        remote(buf, s, fwd, recv, j, partner).wait_recv()
        if onward is not None:
            remote(buf, s, send, recv, 2, onward).start()
        remote(buf, s, fwd, recv, j, partner).start()

    if square:
        arrive(k_buf, k_recv, k_fwd, xn, 1, yn, k_send)
        arrive(v_buf, v_recv, v_fwd, yn, 2, xn, v_send)
        arrive(v_buf, v_recv, v_fwd, xn, 1)
        arrive(k_buf, k_recv, k_fwd, yn, 2)
        attend([xn, yn])
        arrive(k_buf, k_recv, k_fwd, dn, 3)
        arrive(v_buf, v_recv, v_fwd, dn, 3)
        xo, yo, do = xn - 1 + 2 * core, yn - 1 + 2 * core, dn + 1 - 2 * core
        wait_slot(xo)
        wait_slot(yo)
        attend([xo, yo, dn])
        wait_slot(do)
        attend([do])
    else:
        each(1, chips, step)

    for h in range(q_heads):
        here = slice(h * rows, (h + 1) * rows)
        att[:, h * HEAD:(h + 1) * HEAD] = (
            acc[here, :HEAD] / acc[here, HEAD:]
        ).astype(jnp.bfloat16)

    load_w.wait()

    def project(t):
        return jnp.dot(
            att[...], w_buf[:, pl.ds(pl.multiple_of(t * width, width), width)],
            preferred_element_type=jnp.float32,
        )

    def part_copy(j, source, target):
        return pltpu.make_async_remote_copy(
            src_ref=parts.at[j], dst_ref=got.at[source],
            send_sem=p_send.at[j], recv_sem=p_recv.at[source],
            device_id={"tp": target}, device_id_type=MESH,
        )

    def piece_copy(i, dst, recv, target):
        piece = pl.ds(i * (rows // 4), rows // 4)
        return pltpu.make_async_remote_copy(
            src_ref=parts.at[2, piece], dst_ref=dst.at[piece],
            send_sem=p_send.at[2 + i], recv_sem=recv,
            device_id={"tp": target}, device_id_type=MESH,
        )

    if line:
        m0, m1, m2, m3 = (mirror(d) for d in range(4))

        @pl.when(inner == 0)
        def _():
            parts[2] = project(m3).astype(jnp.bfloat16)
            for i in range(4):
                piece_copy(i, relay, r_recv.at[i], m1).start()
            parts[0] = project(m2).astype(jnp.bfloat16)
            part_copy(0, mt, m2).start()
            parts[1] = project(m1).astype(jnp.bfloat16)
            part_copy(1, mt, m1).start()
            total = project(mt)
            part_copy(0, m1, m1).wait_recv()
            total = total + got[m1].astype(jnp.float32)
            for i in range(4):
                piece_copy(i, got.at[m2], r_recv.at[i], m2).wait_recv()
            total = total + got[m2].astype(jnp.float32)
            out_ref[...] = total.astype(out_ref.dtype)

        @pl.when(inner == 1)
        def _():
            parts[0] = project(m2).astype(jnp.bfloat16)
            part_copy(0, mt, m2).start()
            parts[1] = project(m0).astype(jnp.bfloat16)
            part_copy(1, mt, m0).start()
            far = project(m3)
            total = project(mt)
            for i in range(4):
                piece = slice(i * (rows // 4), (i + 1) * (rows // 4))
                piece_copy(i, relay, r_recv.at[i], m0).wait_recv()
                parts[2, piece] = (far[piece] + relay[piece].astype(jnp.float32)).astype(jnp.bfloat16)
                piece_copy(i, got.at[mt], r_recv.at[i], m3).start()
            for source in (m2, m3, m0):
                part_copy(0, source, source).wait_recv()
                total = total + got[source].astype(jnp.float32)
            out_ref[...] = total.astype(out_ref.dtype)

        part_copy(0, mt, m2).wait_send()
        part_copy(1, mt, m0).wait_send()
        for i in range(4):
            piece_copy(i, relay, r_recv.at[i], m1).wait_send()
    else:
        ahead = sorted(range(1, tp), key=lambda j: -min(j, tp - j))
        for j in ahead:
            t = (mt + j) % tp
            parts[j] = project(t).astype(jnp.bfloat16)
            part_copy(j, mt, t).start()
        total = project(mt)
        for j in reversed(ahead):
            source = (mt + j) % tp
            part_copy(j, source, source).wait_recv()
            total = total + got[source].astype(jnp.float32)
        out_ref[...] = total.astype(out_ref.dtype)
        for j in ahead:
            part_copy(j, mt, (mt + j) % tp).wait_send()

    def drain(j):
        remote(k_buf, me, k_send, k_recv, j, peer(j)).wait_send()
        remote(v_buf, me, v_send, v_recv, j, peer(j)).wait_send()

    def drain_fwd(j):
        remote(k_buf, me, k_fwd, k_recv, j, partner).wait_send()
        remote(v_buf, me, v_fwd, v_recv, j, partner).wait_send()

    if square:
        for j in range(3):
            remote(k_buf, me, k_send, k_recv, j, yn).wait_send()
            remote(v_buf, me, v_send, v_recv, j, xn).wait_send()
    else:
        each(1, chips, drain)
    each(0, chips, drain_fwd)


def solution(mesh):
    n, tp = mesh.shape["seq"], mesh.shape["tp"]

    def per_device(queries, keyvalues, stretch_order, block_table, proj_weight):
        rows, q_width = queries.shape
        kv_width = keyvalues.shape[2]
        dout = proj_weight.shape[1]
        q_heads = q_width // HEAD
        dma = pltpu.SemaphoreType.DMA
        return pl.pallas_call(
            functools.partial(kernel, n, tp),
            out_shape=jax.ShapeDtypeStruct((rows, dout // tp), jnp.bfloat16),
            in_specs=[
                pl.BlockSpec(memory_space=pl.ANY),
                pl.BlockSpec(memory_space=pl.ANY),
                pl.BlockSpec(memory_space=pl.ANY),
                pl.BlockSpec(memory_space=pl.ANY),
                pl.BlockSpec(memory_space=pl.ANY),
            ],
            out_specs=pl.BlockSpec(memory_space=pltpu.VMEM),
            scratch_shapes=[
                pltpu.SMEM(stretch_order.shape, jnp.int32),
                pltpu.SMEM(block_table.shape, jnp.int32),
                pltpu.VMEM((rows, q_width), jnp.bfloat16),
                pltpu.VMEM((q_heads * rows, HEAD), jnp.bfloat16),
                pltpu.VMEM((n * rows, kv_width), jnp.bfloat16),
                pltpu.VMEM((n * rows, kv_width), jnp.bfloat16),
                pltpu.VMEM(proj_weight.shape, jnp.bfloat16),
                pltpu.VMEM((q_heads * rows, HEAD), jnp.float32),
                pltpu.VMEM((q_heads * rows, 2 * HEAD), jnp.float32),
                pltpu.VMEM((rows, q_width), jnp.bfloat16),
                pltpu.VMEM((tp, rows, dout // tp), jnp.bfloat16),
                pltpu.VMEM((tp, rows, dout // tp), jnp.bfloat16),
                pltpu.VMEM((rows, dout // tp), jnp.bfloat16),
                dma((6,)),
                dma((n // 2,)), dma((n // 2,)),
                dma((n,)), dma((n,)),
                dma((n // 2,)), dma((n // 2,)),
                dma((max(tp, 6),)), dma((tp,)), dma((4,)),
            ],
            compiler_params=pltpu.CompilerParams(
                collective_id=0, has_side_effects=True,
            ),
        )(queries, keyvalues, stretch_order, block_table, proj_weight)

    return jax.shard_map(
        per_device, mesh=mesh,
        in_specs=(P("seq", "tp"), P(None, "seq", "tp"), P(), P(), P("tp", None)),
        out_specs=P("seq", "tp"), check_vma=False,
    )
```
